16 devices in a mesh: dp: 4 (over z, y), ep: 4 (over x, core).
Axes of the slice: x: 2, y: 2, z: 2, core: 2. Of those that a mesh axis runs over, the one named last changes fastest.
Arguments:
- tokens: bfloat16 [2048, 2048], P(('dp', 'ep')), parts along dimension 0
- routes: int32 [2048, 6], P(('dp', 'ep')), parts along dimension 0
- w_router: bfloat16 [2048, 64], replicated
- w_one: bfloat16 [64, 2048, 1408], P('ep')
- w_three: bfloat16 [64, 2048, 1408], P('ep')
- w_two: bfloat16 [64, 1408, 2048], P('ep')
Outputs:
- output: bfloat16 [2048, 2048], P(('dp', 'ep')), parts along dimension 0
There are 4 independent parts. The reference program is written for one: setup_inputs(seed, part) draws one part's arguments, and reference() takes and returns one part's arrays. A program takes and returns all parts, laid end to end along the dimension named above; an argument that names none is the same for every part.
All inputs are finite; a program needn't handle non-finite values.
Results may differ from the reference program's by a relative error of at most 0.00821994.
Values are sent between devices in bfloat16 or wider.
A program may use at most 1.25 GiB of HBM per device.

```python
import jax
import jax.numpy as jnp
from jax import lax

GROUP_SIZE = 4
DEV_TOKENS = 128
D_MODEL = 2048
D_EXPERT = 1408
NUM_EXPERTS = 64
TOP_K = 6
CAPACITY = 24


def draw_routes(route_key):
    perm_key, row_key, slot_key = jax.random.split(route_key, 3)
    num_pairs = DEV_TOKENS * TOP_K
    hot_count = NUM_EXPERTS // 8
    rest_pairs = num_pairs - hot_count * CAPACITY
    base_count = rest_pairs // (NUM_EXPERTS - hot_count)
    extra_count = rest_pairs % (NUM_EXPERTS - hot_count)
    rank_ids = jnp.arange(NUM_EXPERTS, dtype=jnp.int32)
    counts = jnp.where(rank_ids < hot_count, CAPACITY, base_count + (rank_ids - hot_count < extra_count).astype(jnp.int32))
    count_ends = jnp.cumsum(counts)
    pair_rank = jnp.searchsorted(count_ends, jnp.arange(num_pairs, dtype=jnp.int32), side='right')
    expert_of_rank = jax.random.permutation(perm_key, NUM_EXPERTS)
    layout = expert_of_rank[pair_rank].reshape(TOP_K, DEV_TOKENS).T

    def device_routes(perm_rows, perm_slots):
        row_order = jax.random.permutation(perm_rows, DEV_TOKENS)
        scores = jax.random.randint(perm_slots, (DEV_TOKENS, TOP_K), 0, 1 << 20) * TOP_K + jnp.arange(TOP_K)
        slot_order = jnp.argsort(scores, axis=1)
        return jnp.take_along_axis(layout[row_order], slot_order, axis=1)

    per_device = jax.vmap(device_routes)(jax.random.split(row_key, GROUP_SIZE), jax.random.split(slot_key, GROUP_SIZE))
    return per_device.reshape(GROUP_SIZE * DEV_TOKENS, TOP_K).astype(jnp.int32)


def setup_inputs(seed: int = 0, part: int = 0) -> dict:
    part_key = jax.random.fold_in(jax.random.key(seed), part)
    token_key, route_key = jax.random.split(part_key)
    shared = jax.random.split(jax.random.key(seed + 1), 4)
    tokens = jax.random.normal(token_key, (GROUP_SIZE * DEV_TOKENS, D_MODEL), jnp.float32)
    w_router = jax.random.normal(shared[0], (D_MODEL, NUM_EXPERTS), jnp.float32) * (1.5 * D_MODEL ** -0.5)
    w_one = jax.random.normal(shared[1], (NUM_EXPERTS, D_MODEL, D_EXPERT), jnp.float32) * D_MODEL ** -0.5
    w_three = jax.random.normal(shared[2], (NUM_EXPERTS, D_MODEL, D_EXPERT), jnp.float32) * D_MODEL ** -0.5
    w_two = jax.random.normal(shared[3], (NUM_EXPERTS, D_EXPERT, D_MODEL), jnp.float32) * D_EXPERT ** -0.5
    return {'tokens': tokens.astype(jnp.bfloat16), 'routes': draw_routes(route_key), 'w_router': w_router.astype(jnp.bfloat16), 'w_one': w_one.astype(jnp.bfloat16), 'w_three': w_three.astype(jnp.bfloat16), 'w_two': w_two.astype(jnp.bfloat16)}


def expert_rows(rows, w_gate, w_up, w_down):
    gate_pre = jnp.dot(rows, w_gate, preferred_element_type=jnp.float32)
    up_pre = jnp.dot(rows, w_up, preferred_element_type=jnp.float32)
    hidden = (jax.nn.silu(gate_pre) * up_pre).astype(jnp.bfloat16)
    return jnp.dot(hidden, w_down, preferred_element_type=jnp.float32).astype(jnp.bfloat16)


def reference(tokens, routes, w_router, w_one, w_three, w_two):
    logits = jnp.dot(tokens, w_router, preferred_element_type=jnp.float32)
    gate_vals = jax.nn.softmax(jnp.take_along_axis(logits, routes, axis=1), axis=-1)
    flat_gates = gate_vals.reshape(-1)
    flat_routes = routes.reshape(-1)
    num_pairs = flat_routes.shape[0]
    sort_order = jnp.argsort(flat_routes, stable=True)
    counts = jax.ops.segment_sum(jnp.ones_like(flat_routes), flat_routes, num_segments=NUM_EXPERTS)
    starts = jnp.cumsum(counts) - counts
    slot_ids = jnp.arange(GROUP_SIZE * CAPACITY, dtype=jnp.int32)

    def one_expert(y_sum, step_in):
        w_gate, w_up, w_down, exp_start, exp_count = step_in
        pair_at = sort_order[jnp.minimum(exp_start + slot_ids, num_pairs - 1)]
        token_at = pair_at // TOP_K
        weight = jnp.where(slot_ids < exp_count, flat_gates[pair_at], 0.0)
        out_rows = expert_rows(tokens[token_at], w_gate, w_up, w_down)
        return y_sum.at[token_at].add(weight[:, None] * out_rows.astype(jnp.float32)), None

    y_sum = lax.scan(one_expert, jnp.zeros(tokens.shape, jnp.float32), (w_one, w_three, w_two, starts, counts))[0]
    return y_sum.astype(jnp.bfloat16)
```

```python
import functools

import jax
import jax.numpy as jnp
from jax import lax
from jax.experimental import pallas as pl
from jax.experimental.pallas import tpu as pltpu

MESH = pl.DeviceIdType.MESH
PAD = 32
CC = 512
RING = 6
RING2 = 8
UNROLL = 4


def layer_kernel(tok_hbm, rou_hbm, wr_hbm, w1_hbm, w3_hbm, w2_hbm, y_hbm,
                 w13, w2r, tok, meta, code, pg, xbuf, hid, obuf, wr, rou,
                 stage, xsend, own, rec_agg, rec_fin, rec_x, ybuf,
                 w13_sem, w2_sem, in_sem, out_sem,
                 tok_ss, tok_rs, meta_ss, meta_rs, ret_ss, ret_rs):
    me = lax.axis_index('ep')
    core = lax.rem(me, 2)
    sib = me + 1 - 2 * core
    far = lax.rem(me + 2, 4)
    diag = far + 1 - 2 * core
    n_tok, d_model = tok_hbm.shape
    n_exp = wr_hbm.shape[1]
    n_loc, _, d_ff = w1_hbm.shape
    n_chunk = d_model // CC
    rows = 4 * PAD
    f32, bf16 = jnp.float32, jnp.bfloat16

    def w1_copy(e, slot):
        return pltpu.make_async_copy(w1_hbm.at[e], w13.at[slot], w13_sem.at[slot])

    def w3_copy(e, slot):
        return pltpu.make_async_copy(w3_hbm.at[e], w13.at[slot], w13_sem.at[slot])

    def w2_copy(q, slot):
        c = lax.div(q, n_loc)
        e = lax.rem(q, n_loc)
        cols = pl.ds(pl.multiple_of(c * CC, CC), CC)
        return pltpu.make_async_copy(w2_hbm.at[e, :, cols], w2r.at[slot], w2_sem.at[slot])

    tok_in = pltpu.make_async_copy(tok_hbm, tok.at[me], in_sem.at[0])
    rou_in = pltpu.make_async_copy(rou_hbm, rou, in_sem.at[1])
    wr_in = pltpu.make_async_copy(wr_hbm, wr, in_sem.at[2])
    tok_in.start()
    rou_in.start()
    wr_in.start()
    for k in range(RING // 2):
        w1_copy(k, 2 * k).start()
        w3_copy(k, 2 * k + 1).start()
    for k in range(RING2):
        w2_copy(k, k).start()

    barrier = pltpu.get_barrier_semaphore()
    for peer in (sib, far):
        pl.semaphore_signal(barrier, inc=1, device_id={'ep': peer}, device_id_type=MESH)
    pl.semaphore_wait(barrier, 2)

    def send(src, dst, ss, rs, peer):
        return pltpu.make_async_remote_copy(src_ref=src, dst_ref=dst, send_sem=ss, recv_sem=rs,
                                            device_id={'ep': peer}, device_id_type=MESH)

    tok_far = send(tok.at[me], tok.at[me], tok_ss.at[0], tok_rs.at[0], far)
    tok_sib = send(tok.at[me], tok.at[me], tok_ss.at[1], tok_rs.at[1], sib)
    tok_fwd = send(tok.at[far], tok.at[far], tok_ss.at[2], tok_rs.at[2], sib)
    meta_far = send(meta.at[me], meta.at[me], meta_ss.at[0], meta_rs.at[0], far)
    meta_sib = send(meta.at[me], meta.at[me], meta_ss.at[1], meta_rs.at[1], sib)
    meta_fwd = send(meta.at[far], meta.at[far], meta_ss.at[2], meta_rs.at[2], sib)
    tok_in.wait()
    tok_far.start()
    tok_sib.start()

    rou_in.wait()
    wr_in.wait()
    lane = lax.broadcasted_iota(jnp.int32, (n_tok, 2 * n_exp), 1)
    named = lane == rou[:, 0:1]
    for j in range(1, rou.shape[1]):
        named = jnp.logical_or(named, lane == rou[:, j:j + 1])
    logits = jnp.dot(tok[me], wr[...], preferred_element_type=f32)
    logits = jnp.concatenate([logits, logits], axis=1)
    top = jnp.max(jnp.where(named, logits, -jnp.inf), axis=1, keepdims=True)
    ex = jnp.exp(jnp.where(named, logits - top, -jnp.inf))
    gates = ex / jnp.sum(ex, axis=1, keepdims=True)
    meta[me] = jnp.transpose(jnp.where(named, gates, -1.0))[:n_exp, :]
    before = (lax.broadcasted_iota(jnp.int32, (n_tok, n_tok), 0)
              < lax.broadcasted_iota(jnp.int32, (n_tok, n_tok), 1)).astype(f32).astype(bf16)
    meta_far.start()
    meta_sib.start()
    tok_far.wait_recv()
    tok_fwd.start()
    meta_far.wait_recv()
    meta_fwd.start()
    tok_sib.wait_recv()
    meta_sib.wait_recv()
    meta_fwd.wait_recv()

    base = pl.multiple_of(me * n_loc, n_loc)
    slot_r = lax.broadcasted_iota(jnp.int32, (n_loc, PAD, n_tok), 1).astype(f32)
    for s in range(4):
        g = meta[s, pl.ds(base, n_loc), :]
        on = g >= 0.0
        rank = jnp.dot(on.astype(f32).astype(bf16), before, preferred_element_type=f32)
        code[:, s * n_tok:(s + 1) * n_tok] = jnp.where(on, rank + float(s * PAD), -1.0)
        rank = jnp.where(on, rank, -1.0)
        w = jnp.where(rank[:, None, :] == slot_r, g[:, None, :], 0.0)
        w = jnp.transpose(w.reshape(n_loc * PAD, n_tok))
        hi = w.astype(bf16)
        w = w - hi.astype(f32)
        mid = w.astype(bf16)
        w = w - mid.astype(f32)
        pg[s, 0:n_tok, :] = hi
        pg[s, n_tok:2 * n_tok, :] = mid
        pg[s, 2 * n_tok:3 * n_tok, :] = w.astype(bf16)
    tok_fwd.wait_recv()

    row_id = lax.broadcasted_iota(jnp.int32, (rows, 4 * n_tok), 0).astype(f32)
    tok_all = tok.reshape(4 * n_tok, d_model)

    def up(e, _):
        pick = jnp.where(code[pl.ds(e, 1), :] == row_id, 1.0, 0.0).astype(bf16)
        for n in range(0, d_model, 512):
            xbuf[:, n:n + 512] = jnp.dot(pick, tok_all[:, n:n + 512], preferred_element_type=f32).astype(bf16)
        s1 = lax.rem(2 * e, RING)
        s3 = lax.rem(2 * e + 1, RING)
        w1_copy(e, s1).wait()
        w3_copy(e, s3).wait()
        for n in range(0, d_ff, 256):
            m = min(n + 256, d_ff)
            a = jnp.dot(xbuf[...], w13[s1, :, n:m], preferred_element_type=f32)
            b = jnp.dot(xbuf[...], w13[s3, :, n:m], preferred_element_type=f32)
            hid[e, :, n:m] = (a / (1.0 + jnp.exp(-a)) * b).astype(bf16)

        @pl.when(e + RING // 2 < n_loc)
        def _():
            w1_copy(e + RING // 2, s1).start()
            w3_copy(e + RING // 2, s3).start()
        return 0

    lax.fori_loop(0, n_loc, up, 0)

    def agg_in(c):
        return send(stage.at[0], rec_agg.at[c], ret_ss.at[0, c], ret_rs.at[0, c], sib)

    def fin_in(c):
        return send(stage.at[1], rec_fin.at[c], ret_ss.at[1, c], ret_rs.at[1, c], sib)

    def x_in(c):
        return send(xsend.at[c], rec_x.at[c], ret_ss.at[2, c], ret_rs.at[2, c], far)

    def forward(c):
        agg_in(c).wait()
        xsend[c] = xsend[c] + rec_agg[c]
        x_in(c).start()
        fin_in(c).wait_send()

    def part(s):
        o = obuf[:, pl.ds(pl.multiple_of(s * PAD, PAD), PAD), :].reshape(n_loc * PAD, CC)
        p = jnp.dot(pg[s], o, preferred_element_type=f32)
        return p[:n_tok] + p[n_tok:2 * n_tok] + p[2 * n_tok:]

    n_q = n_chunk * n_loc

    def down(c, _):
        def some(i, _):
            for k in range(UNROLL):
                e = i * UNROLL + k
                q = c * n_loc + e
                w2_copy(q, lax.rem(q, RING2)).wait()
            for k in range(UNROLL):
                e = i * UNROLL + k
                q = c * n_loc + e
                obuf[e] = jnp.dot(hid[e], w2r[lax.rem(q, RING2)], preferred_element_type=f32).astype(bf16)
            for k in range(UNROLL):
                q = c * n_loc + i * UNROLL + k

                @pl.when(q + RING2 < n_q)
                def _():
                    w2_copy(q + RING2, lax.rem(q, RING2)).start()
            return 0

        lax.fori_loop(0, n_loc // UNROLL, some, 0)

        @pl.when(c > 0)
        def _():
            forward(c - 1)
        stage[0] = part(diag)
        stage[1] = part(sib)
        agg_in(c).start()
        fin_in(c).start()
        xsend[c] = part(far)
        own[c] = part(me)
        return 0

    lax.fori_loop(0, n_chunk, down, 0)
    forward(n_chunk - 1)

    for c in range(n_chunk):
        fin_in(c).wait_recv()
        x_in(c).wait_recv()
        ybuf[:, c * CC:(c + 1) * CC] = (own[c] + rec_fin[c] + rec_x[c]).astype(bf16)
    y_out = pltpu.make_async_copy(ybuf, y_hbm, out_sem.at[0])
    y_out.start()
    for c in range(n_chunk):
        x_in(c).wait_send()
    for copy in (tok_far, tok_sib, tok_fwd, meta_far, meta_sib, meta_fwd):
        copy.wait_send()
    y_out.wait()


def solution(mesh):
    row_spec = jax.sharding.PartitionSpec(('dp', 'ep'), None)
    expert_spec = jax.sharding.PartitionSpec('ep', None, None)

    def device_step(tokens, routes, w_router, w_one, w_three, w_two):
        n_tok, d_model = tokens.shape
        n_loc, _, d_ff = w_one.shape
        n_exp = w_router.shape[1]
        n_chunk = d_model // CC
        any_spec = pl.BlockSpec(memory_space=pl.ANY)
        f32, bf16 = jnp.float32, jnp.bfloat16
        flops = 2 * n_loc * 4 * PAD * d_model * d_ff * 3
        return pl.pallas_call(
            layer_kernel,
            out_shape=jax.ShapeDtypeStruct((n_tok, d_model), bf16),
            in_specs=[any_spec] * 6,
            out_specs=any_spec,
            scratch_shapes=[
                pltpu.VMEM((RING, d_model, d_ff), bf16),
                pltpu.VMEM((RING2, d_ff, CC), bf16),
                pltpu.VMEM((4, n_tok, d_model), bf16),
                pltpu.VMEM((4, n_exp, n_tok), f32),
                pltpu.VMEM((n_loc, 4 * n_tok), f32),
                pltpu.VMEM((4, 3 * n_tok, n_loc * PAD), bf16),
                pltpu.VMEM((4 * PAD, d_model), bf16),
                pltpu.VMEM((n_loc, 4 * PAD, d_ff), bf16),
                pltpu.VMEM((n_loc, 4 * PAD, CC), bf16),
                pltpu.VMEM(w_router.shape, bf16),
                pltpu.VMEM(routes.shape, jnp.int32),
                pltpu.VMEM((2, n_tok, CC), f32),
                pltpu.VMEM((n_chunk, n_tok, CC), f32),
                pltpu.VMEM((n_chunk, n_tok, CC), f32),
                pltpu.VMEM((n_chunk, n_tok, CC), f32),
                pltpu.VMEM((n_chunk, n_tok, CC), f32),
                pltpu.VMEM((n_chunk, n_tok, CC), f32),
                pltpu.VMEM((n_tok, d_model), bf16),
                pltpu.SemaphoreType.DMA((RING,)),
                pltpu.SemaphoreType.DMA((RING2,)),
                pltpu.SemaphoreType.DMA((3,)),
                pltpu.SemaphoreType.DMA((1,)),
                pltpu.SemaphoreType.DMA((3,)),
                pltpu.SemaphoreType.DMA((3,)),
                pltpu.SemaphoreType.DMA((3,)),
                pltpu.SemaphoreType.DMA((3,)),
                pltpu.SemaphoreType.DMA((3, n_chunk)),
                pltpu.SemaphoreType.DMA((3, n_chunk)),
            ],
            compiler_params=pltpu.CompilerParams(collective_id=0, has_side_effects=True,
                                                 vmem_limit_bytes=67043328),
            cost_estimate=pl.CostEstimate(flops=flops, bytes_accessed=2 * n_loc * d_model * d_ff * 3, transcendentals=0),
        )(tokens, routes, w_router, w_one, w_three, w_two)

    return jax.shard_map(device_step, mesh=mesh, in_specs=(row_spec, row_spec, jax.sharding.PartitionSpec(None, None),
                                                           expert_spec, expert_spec, expert_spec),
                         out_specs=row_spec, check_vma=False)
```

```python
import functools

import jax
import jax.numpy as jnp
from jax import lax
from jax.experimental import pallas as pl
from jax.experimental.pallas import tpu as pltpu

MESH = pl.DeviceIdType.MESH
PAD = 32
CC = 512
RING = 6
RING2 = 8
UNROLL = 4


def layer_kernel(tok_hbm, rou_hbm, wr_hbm, w1_hbm, w3_hbm, w2_hbm, y_hbm,
                 w13, w2r, tok, meta, code, pg, xbuf, hid, obuf, wr, rou,
                 stage, xsend, own, rec_agg, rec_fin, rec_x, ybuf,
                 w13_sem, w2_sem, in_sem, out_sem,
                 tok_ss, tok_rs, meta_ss, meta_rs, ret_ss, ret_rs):
    me = lax.axis_index('ep')
    core = lax.rem(me, 2)
    sib = me + 1 - 2 * core
    far = lax.rem(me + 2, 4)
    diag = far + 1 - 2 * core
    n_tok, d_model = tok_hbm.shape
    n_exp = wr_hbm.shape[0]
    n_loc, _, d_ff = w1_hbm.shape
    n_chunk = d_model // CC
    rows = 4 * PAD
    f32, bf16 = jnp.float32, jnp.bfloat16

    def w1_copy(e, slot):
        return pltpu.make_async_copy(w1_hbm.at[e], w13.at[slot], w13_sem.at[slot])

    def w3_copy(e, slot):
        return pltpu.make_async_copy(w3_hbm.at[e], w13.at[slot], w13_sem.at[slot])

    def w2_copy(q, slot):
        c = lax.div(q, n_loc)
        e = lax.rem(q, n_loc)
        cols = pl.ds(pl.multiple_of(c * CC, CC), CC)
        return pltpu.make_async_copy(w2_hbm.at[e, :, cols], w2r.at[slot], w2_sem.at[slot])

    tok_in = pltpu.make_async_copy(tok_hbm, tok.at[me], in_sem.at[0])
    rou_in = pltpu.make_async_copy(rou_hbm, rou, in_sem.at[1])
    wr_in = pltpu.make_async_copy(wr_hbm, wr, in_sem.at[2])
    tok_in.start()
    rou_in.start()
    wr_in.start()
    tok_in.wait()
    rou_in.wait()
    wr_in.wait()
    for k in range(RING // 2):
        w1_copy(k, 2 * k).start()
        w3_copy(k, 2 * k + 1).start()
    for k in range(RING2):
        w2_copy(k, k).start()

    barrier = pltpu.get_barrier_semaphore()
    for peer in (sib, far):
        pl.semaphore_signal(barrier, inc=1, device_id={'ep': peer}, device_id_type=MESH)
    pl.semaphore_wait(barrier, 2)

    def send(src, dst, ss, rs, peer):
        return pltpu.make_async_remote_copy(src_ref=src, dst_ref=dst, send_sem=ss, recv_sem=rs,
                                            device_id={'ep': peer}, device_id_type=MESH)

    tok_far = send(tok.at[me], tok.at[me], tok_ss.at[0], tok_rs.at[0], far)
    tok_sib = send(tok.at[me], tok.at[me], tok_ss.at[1], tok_rs.at[1], sib)
    tok_fwd = send(tok.at[far], tok.at[far], tok_ss.at[2], tok_rs.at[2], sib)
    meta_far = send(meta.at[me], meta.at[me], meta_ss.at[0], meta_rs.at[0], far)
    meta_sib = send(meta.at[me], meta.at[me], meta_ss.at[1], meta_rs.at[1], sib)
    meta_fwd = send(meta.at[far], meta.at[far], meta_ss.at[2], meta_rs.at[2], sib)
    tok_far.start()
    tok_sib.start()

    expert = lax.broadcasted_iota(jnp.int32, (n_exp, n_tok), 0)
    named = expert == rou[0:1, :]
    for j in range(1, rou.shape[0]):
        named = jnp.logical_or(named, expert == rou[j:j + 1, :])
    logits = lax.dot_general(wr[...], tok[me], (((1,), (1,)), ((), ())), preferred_element_type=f32)
    top = jnp.max(jnp.where(named, logits, -jnp.inf), axis=0, keepdims=True)
    ex = jnp.exp(jnp.where(named, logits - top, -jnp.inf))
    gates = ex / jnp.sum(ex, axis=0, keepdims=True)
    meta[me] = jnp.where(named, gates, -1.0)
    before = (lax.broadcasted_iota(jnp.int32, (n_tok, n_tok), 0)
              < lax.broadcasted_iota(jnp.int32, (n_tok, n_tok), 1)).astype(f32).astype(bf16)
    meta_far.start()
    meta_sib.start()
    tok_far.wait_recv()
    tok_fwd.start()
    meta_far.wait_recv()
    meta_fwd.start()
    tok_sib.wait_recv()
    meta_sib.wait_recv()
    meta_fwd.wait_recv()

    base = pl.multiple_of(me * n_loc, n_loc)
    slot_r = lax.broadcasted_iota(jnp.int32, (n_loc, PAD, n_tok), 1).astype(f32)
    for s in range(4):
        g = meta[s, pl.ds(base, n_loc), :]
        on = g >= 0.0
        rank = jnp.dot(on.astype(f32).astype(bf16), before, preferred_element_type=f32)
        code[:, s * n_tok:(s + 1) * n_tok] = jnp.where(on, rank + float(s * PAD), -1.0)
        rank = jnp.where(on, rank, -1.0)
        w = jnp.where(rank[:, None, :] == slot_r, g[:, None, :], 0.0)
        w = jnp.transpose(w.reshape(n_loc * PAD, n_tok))
        hi = w.astype(bf16)
        w = w - hi.astype(f32)
        mid = w.astype(bf16)
        w = w - mid.astype(f32)
        pg[s, 0:n_tok, :] = hi
        pg[s, n_tok:2 * n_tok, :] = mid
        pg[s, 2 * n_tok:3 * n_tok, :] = w.astype(bf16)
    tok_fwd.wait_recv()

    row_id = lax.broadcasted_iota(jnp.int32, (rows, 4 * n_tok), 0).astype(f32)
    tok_all = tok.reshape(4 * n_tok, d_model)

    def up(e, _):
        pick = jnp.where(code[pl.ds(e, 1), :] == row_id, 1.0, 0.0).astype(bf16)
        for n in range(0, d_model, 512):
            xbuf[:, n:n + 512] = jnp.dot(pick, tok_all[:, n:n + 512], preferred_element_type=f32).astype(bf16)
        s1 = lax.rem(2 * e, RING)
        s3 = lax.rem(2 * e + 1, RING)
        w1_copy(e, s1).wait()
        w3_copy(e, s3).wait()
        for n in range(0, d_ff, 256):
            m = min(n + 256, d_ff)
            a = jnp.dot(xbuf[...], w13[s1, :, n:m], preferred_element_type=f32)
            b = jnp.dot(xbuf[...], w13[s3, :, n:m], preferred_element_type=f32)
            hid[e, :, n:m] = (a / (1.0 + jnp.exp(-a)) * b).astype(bf16)

        @pl.when(e + RING // 2 < n_loc)
        def _():
            w1_copy(e + RING // 2, s1).start()
            w3_copy(e + RING // 2, s3).start()
        return 0

    lax.fori_loop(0, n_loc, up, 0)

    def agg_in(c):
        return send(stage.at[0], rec_agg.at[c], ret_ss.at[0, c], ret_rs.at[0, c], sib)

    def fin_in(c):
        return send(stage.at[1], rec_fin.at[c], ret_ss.at[1, c], ret_rs.at[1, c], sib)

    def x_in(c):
        return send(xsend.at[c], rec_x.at[c], ret_ss.at[2, c], ret_rs.at[2, c], far)

    def forward(c):
        agg_in(c).wait()
        xsend[c] = xsend[c] + rec_agg[c]
        x_in(c).start()
        fin_in(c).wait_send()

    def part(s):
        o = obuf[:, pl.ds(pl.multiple_of(s * PAD, PAD), PAD), :].reshape(n_loc * PAD, CC)
        p = jnp.dot(pg[s], o, preferred_element_type=f32)
        return p[:n_tok] + p[n_tok:2 * n_tok] + p[2 * n_tok:]

    n_q = n_chunk * n_loc

    def down(c, _):
        def some(i, _):
            for k in range(UNROLL):
                e = i * UNROLL + k
                q = c * n_loc + e
                w2_copy(q, lax.rem(q, RING2)).wait()
            for k in range(UNROLL):
                e = i * UNROLL + k
                q = c * n_loc + e
                obuf[e] = jnp.dot(hid[e], w2r[lax.rem(q, RING2)], preferred_element_type=f32).astype(bf16)
            for k in range(UNROLL):
                q = c * n_loc + i * UNROLL + k

                @pl.when(q + RING2 < n_q)
                def _():
                    w2_copy(q + RING2, lax.rem(q, RING2)).start()
            return 0

        some(0, 0)

        @pl.when(c > 0)
        def _():
            forward(c - 1)
        lax.fori_loop(1, n_loc // UNROLL, some, 0)

        stage[0] = part(diag)
        stage[1] = part(sib)
        agg_in(c).start()
        fin_in(c).start()
        xsend[c] = part(far)
        own[c] = part(me)
        return 0

    lax.fori_loop(0, n_chunk, down, 0)
    forward(n_chunk - 1)

    for c in range(n_chunk):
        fin_in(c).wait_recv()
        x_in(c).wait_recv()
        ybuf[:, c * CC:(c + 1) * CC] = (own[c] + rec_fin[c] + rec_x[c]).astype(bf16)
    y_out = pltpu.make_async_copy(ybuf, y_hbm, out_sem.at[0])
    y_out.start()
    for c in range(n_chunk):
        x_in(c).wait_send()
    for copy in (tok_far, tok_sib, tok_fwd, meta_far, meta_sib, meta_fwd):
        copy.wait_send()
    y_out.wait()


def solution(mesh):
    row_spec = jax.sharding.PartitionSpec(('dp', 'ep'), None)
    expert_spec = jax.sharding.PartitionSpec('ep', None, None)

    def device_step(tokens, routes, w_router, w_one, w_three, w_two):
        n_tok, d_model = tokens.shape
        n_loc, _, d_ff = w_one.shape
        n_exp = w_router.shape[1]
        n_chunk = d_model // CC
        any_spec = pl.BlockSpec(memory_space=pl.ANY)
        f32, bf16 = jnp.float32, jnp.bfloat16
        flops = 2 * n_loc * 4 * PAD * d_model * d_ff * 3
        return pl.pallas_call(
            layer_kernel,
            out_shape=jax.ShapeDtypeStruct((n_tok, d_model), bf16),
            in_specs=[any_spec] * 6,
            out_specs=any_spec,
            scratch_shapes=[
                pltpu.VMEM((RING, d_model, d_ff), bf16),
                pltpu.VMEM((RING2, d_ff, CC), bf16),
                pltpu.VMEM((4, n_tok, d_model), bf16),
                pltpu.VMEM((4, n_exp, n_tok), f32),
                pltpu.VMEM((n_loc, 4 * n_tok), f32),
                pltpu.VMEM((4, 3 * n_tok, n_loc * PAD), bf16),
                pltpu.VMEM((4 * PAD, d_model), bf16),
                pltpu.VMEM((n_loc, 4 * PAD, d_ff), bf16),
                pltpu.VMEM((n_loc, 4 * PAD, CC), bf16),
                pltpu.VMEM((n_exp, d_model), bf16),
                pltpu.VMEM(routes.shape[::-1], jnp.int32),
                pltpu.VMEM((2, n_tok, CC), f32),
                pltpu.VMEM((n_chunk, n_tok, CC), f32),
                pltpu.VMEM((n_chunk, n_tok, CC), f32),
                pltpu.VMEM((n_chunk, n_tok, CC), f32),
                pltpu.VMEM((n_chunk, n_tok, CC), f32),
                pltpu.VMEM((n_chunk, n_tok, CC), f32),
                pltpu.VMEM((n_tok, d_model), bf16),
                pltpu.SemaphoreType.DMA((RING,)),
                pltpu.SemaphoreType.DMA((RING2,)),
                pltpu.SemaphoreType.DMA((3,)),
                pltpu.SemaphoreType.DMA((1,)),
                pltpu.SemaphoreType.DMA((3,)),
                pltpu.SemaphoreType.DMA((3,)),
                pltpu.SemaphoreType.DMA((3,)),
                pltpu.SemaphoreType.DMA((3,)),
                pltpu.SemaphoreType.DMA((3, n_chunk)),
                pltpu.SemaphoreType.DMA((3, n_chunk)),
            ],
            compiler_params=pltpu.CompilerParams(collective_id=0, has_side_effects=True,
                                                 vmem_limit_bytes=67043328),
            cost_estimate=pl.CostEstimate(flops=flops, bytes_accessed=2 * n_loc * d_model * d_ff * 3, transcendentals=0),
        )(tokens, routes.T, w_router.T, w_one, w_three, w_two)

    return jax.shard_map(device_step, mesh=mesh, in_specs=(row_spec, row_spec, jax.sharding.PartitionSpec(None, None),
                                                           expert_spec, expert_spec, expert_spec),
                         out_specs=row_spec, check_vma=False)
```
